32 devices in a mesh: rep: 8 (over y, x, core), tp: 4 (over z).
Axes of the slice: x: 2, y: 2, z: 4, core: 2. Of those that a mesh axis runs over, the one named last changes fastest.
Arguments:
- tokens: bfloat16 [8192, 1280], P(('rep', 'tp')), may hold values from -6 to 6
- view_ids: int32 [32, 4], P('rep'), may hold values from 0 to 31
- time_ids: int32 [32], P('rep'), may hold values from 0 to 999
- camera_table: float32 [32, 1280], replicated, may hold values from -6 to 6
- norm_attn: float32 [2, 1280], replicated, may hold values from 0.1 to 1.9
- norm_ffn: float32 [2, 1280], replicated, may hold values from 0.1 to 1.9
- w_query: bfloat16 [2, 1280, 1280], P(None, ('rep', 'tp')), may hold values from -0.1677051 to 0.1677051
- w_key: bfloat16 [2, 1280, 1280], P(None, ('rep', 'tp')), may hold values from -6.764106 to 6.764106
- w_value: bfloat16 [2, 1280, 1280], P(None, ('rep', 'tp')), may hold values from -0.15625 to 0.15625
- w_out: bfloat16 [2, 1280, 1280], P(None, ('rep', 'tp')), may hold values from -0.15625 to 0.15625
- w_gate: bfloat16 [2, 1280, 5120], P(None, ('rep', 'tp')), may hold values from -0.15625 to 0.15625
- w_up: bfloat16 [2, 1280, 5120], P(None, ('rep', 'tp')), may hold values from -0.15625 to 0.15625
- w_down: bfloat16 [2, 1280, 5120], P(None, ('rep', 'tp')), may hold values from -0.078125 to 0.078125
Outputs:
- denoised: bfloat16 [8192, 1280], P(('rep', 'tp'))
The draws below stay inside these ranges and needn't reach their ends.
All inputs are finite; a program needn't handle non-finite values.
Results may differ from the reference program's by a relative error of at most 0.035.
Values may be sent and summed in bfloat16 or wider, within the bound.
A program may use at most 128 MiB of HBM per device.

```python
import math
import jax
import jax.numpy as jnp
from jax import lax

D = 1280
FF = 5120
HEADS = 8
VIEWS = 4
HW = 64
LAYERS = 2
NPOSE = 32
CAMS = 32
ROWS = 8192
N_TP = 4


def query_base(key):
    base = jax.random.normal(jax.random.fold_in(key, 11), (LAYERS, D, D), jnp.float32)
    return jnp.clip(base, -6.0, 6.0) * D ** (-0.5)


def draw_w_query(key, part):
    return query_base(key).astype(jnp.bfloat16)


def draw_w_key(key, part):
    other = jax.random.normal(jax.random.fold_in(key, 12), (LAYERS, D, D), jnp.float32)
    other = jnp.clip(other, -6.0, 6.0) * D ** (-0.5)
    return other.astype(jnp.bfloat16)


def touch_ends(drawn, own_key, low, high):
    dims = drawn.shape
    spot = [jax.random.randint(jax.random.fold_in(own_key, axis), (), 0, dims[axis]) for axis in range(len(dims))]
    drawn = drawn.at[tuple(spot)].set(low)
    longest = dims.index(max(dims))
    spot[longest] = (spot[longest] + 1) % dims[longest]
    return drawn.at[tuple(spot)].set(high)


def block_scale(rng, dims, shards, smallest, top_value):
    loudness = 1.0
    for dim, parts in shards:
        draws = jax.random.uniform(jax.random.fold_in(jax.random.fold_in(rng, 6), dim), (parts,), jnp.float32, smallest / len(shards), top_value / len(shards))
        loudness = loudness * jnp.repeat(jnp.exp(draws), dims[dim] // parts).reshape((-1,) + (1,) * (len(dims) - 1 - dim))
    return loudness


def gaussian(key, shape, scale, limit, shards=(), kind=jnp.bfloat16):
    values = jax.random.normal(key, shape, jnp.float32) * scale
    if len(shards) > 0:
        values = block_scale(key, shape, shards, -0.22, 0.18) * values
    return jnp.clip(values, min=-limit, max=limit).astype(kind)


def setup_inputs(seed: int = 0) -> dict:
    streams_of = jax.random.split(jax.random.key(seed), 14)
    tokens = gaussian(streams_of[0], (ROWS, D), 1.0, 6.0, ((0, 32),))
    view_ids = touch_ends(jax.random.randint(streams_of[1], (CAMS, VIEWS), 0, NPOSE), jax.random.fold_in(streams_of[1], 1), 0, NPOSE - 1).astype(jnp.int32)
    time_ids = touch_ends(jax.random.randint(streams_of[2], (CAMS,), 0, 1000), jax.random.fold_in(streams_of[2], 1), 0, 999).astype(jnp.int32)
    camera_table = gaussian(streams_of[3], (NPOSE, D), 1.0, 6.0, (), jnp.float32)
    norm_attn = jnp.clip(1.0 + 0.18 * jax.random.normal(streams_of[4], (LAYERS, D), jnp.float32), 0.1, 1.9)
    norm_ffn = jnp.clip(1.0 + 0.18 * jax.random.normal(streams_of[5], (LAYERS, D), jnp.float32), 0.1, 1.9)
    w_query = draw_w_query(jax.random.fold_in(streams_of[13], 71), 0)
    w_key = draw_w_key(jax.random.fold_in(streams_of[13], 71), 0)
    w_value = gaussian(streams_of[8], (LAYERS, D, D), D ** -0.5, 0.15625, ((1, 32),))
    w_out = gaussian(streams_of[9], (LAYERS, D, D), D ** -0.5, 0.15625, ((1, 32),))
    w_gate = gaussian(streams_of[10], (LAYERS, D, FF), D ** -0.5, 0.15625, ((1, 32),))
    w_up = gaussian(streams_of[11], (LAYERS, D, FF), D ** -0.5, 0.15625, ((1, 32),))
    w_down = gaussian(streams_of[12], (LAYERS, D, FF), FF ** -0.5, 0.078125, ((1, 32),))
    return dict(tokens=tokens, view_ids=view_ids, time_ids=time_ids, camera_table=camera_table, norm_attn=norm_attn, norm_ffn=norm_ffn, w_query=w_query, w_key=w_key, w_value=w_value, w_out=w_out, w_gate=w_gate, w_up=w_up, w_down=w_down)


def layer_norm(activations, gain_vector):
    average = lax.optimization_barrier(jnp.mean(activations, axis=-1, keepdims=True))
    centred = activations - average
    spread = lax.optimization_barrier(jnp.mean(centred * centred, axis=-1, keepdims=True))
    return (centred * lax.rsqrt(spread + 1e-05) * gain_vector).astype(jnp.bfloat16)

def time_code(step_ids, width):
    half_width = width // 2
    frequency = jnp.exp(-math.log(10000.0) * jnp.arange(half_width, dtype=jnp.float32) / half_width)
    angles = step_ids.astype(jnp.float32)[:, None] * frequency[None, :]
    return jnp.concatenate([jnp.cos(angles), jnp.sin(angles)], axis=1)

def split_sum(mixed_rows, weight):
    row_count = mixed_rows.shape[0]
    inner_width = mixed_rows.shape[1] // N_TP
    left_side = mixed_rows.astype(jnp.float32).reshape(row_count, N_TP, inner_width)
    right_side = weight.astype(jnp.float32).reshape(weight.shape[0], N_TP, inner_width)
    term_rows = jnp.einsum('snc,onc->nso', left_side, right_side).astype(jnp.bfloat16)
    term_rows = lax.optimization_barrier(term_rows)
    return lax.optimization_barrier(jnp.sum(term_rows.astype(jnp.float32), axis=0))

def attention(query_rows, key_rows, value_rows):
    seq_len = query_rows.shape[0]
    head_size = D // HEADS
    query_heads = query_rows.astype(jnp.float32).reshape(seq_len, HEADS, head_size)
    key_heads = key_rows.astype(jnp.float32).reshape(seq_len, HEADS, head_size)
    value_heads = value_rows.astype(jnp.float32).reshape(seq_len, HEADS, head_size)
    scores = jnp.einsum('qhd,khd->hqk', query_heads, key_heads) * head_size ** (-0.5)
    peak = lax.optimization_barrier(jnp.max(scores, axis=-1, keepdims=True))
    expons = jnp.exp(scores - peak)
    attn_probs = (expons / lax.optimization_barrier(jnp.sum(expons, axis=-1, keepdims=True))).astype(jnp.bfloat16)
    mixed_rows = jnp.einsum('hqk,khd->qhd', attn_probs.astype(jnp.float32), value_heads)
    return mixed_rows.astype(jnp.bfloat16).reshape(seq_len, D)

def reference(tokens, view_ids, time_ids, camera_table, norm_attn, norm_ffn, w_query, w_key, w_value, w_out, w_gate, w_up, w_down):
    seq_len = VIEWS * HW
    set_count = tokens.shape[0] // seq_len
    blocks = tokens.reshape(set_count, seq_len, D)

    def one_set(packed):
        block, views_here, step_here = packed
        camera = jnp.repeat(camera_table[views_here], HW, axis=0)
        stream = block.astype(jnp.float32) + camera + time_code(step_here[None], D)
        for layer_index in range(LAYERS):
            normed = layer_norm(stream, norm_attn[layer_index])
            query_rows = jnp.dot(normed, w_query[layer_index], preferred_element_type=jnp.float32).astype(jnp.bfloat16)
            key_rows = jnp.dot(normed, w_key[layer_index], preferred_element_type=jnp.float32).astype(jnp.bfloat16)
            value_rows = jnp.dot(normed, w_value[layer_index], preferred_element_type=jnp.float32).astype(jnp.bfloat16)
            mixed_rows = attention(query_rows, key_rows, value_rows)
            stream = stream + split_sum(mixed_rows, w_out[layer_index])
            normed = layer_norm(stream, norm_ffn[layer_index])
            gate_part = jnp.dot(normed, w_gate[layer_index], preferred_element_type=jnp.float32)
            up_part = jnp.dot(normed, w_up[layer_index], preferred_element_type=jnp.float32)
            hidden = (jax.nn.gelu(gate_part, approximate=False) * up_part).astype(jnp.bfloat16)
            stream = stream + split_sum(hidden, w_down[layer_index])
        return stream.astype(jnp.bfloat16)
    result = lax.map(one_set, (blocks, view_ids, time_ids))
    return result.reshape(tokens.shape[0], D)
```

```python
import functools
import math

import jax
import jax.numpy as jnp
from jax import lax
from jax.experimental import pallas as pl
from jax.experimental.pallas import tpu as pltpu
from jax.sharding import PartitionSpec as P

D = 1280
HEADS = 8
VIEWS = 4
HW = 64
LAYERS = 2


def layer_norm(activations, gain_vector):
    average = jnp.mean(activations, axis=-1, keepdims=True)
    centred = activations - average
    spread = jnp.mean(centred * centred, axis=-1, keepdims=True)
    return (centred * lax.rsqrt(spread + 1e-05) * gain_vector).astype(jnp.bfloat16)


def time_code(step_ids, width):
    half_width = width // 2
    frequency = jnp.exp(-math.log(10000.0) * jnp.arange(half_width, dtype=jnp.float32) / half_width)
    angles = step_ids.astype(jnp.float32)[:, None] * frequency[None, :]
    return jnp.concatenate([jnp.cos(angles), jnp.sin(angles)], axis=1)


def conditioning(row_ids, view_ids, time_ids, camera_table):
    set_ids = row_ids // (VIEWS * HW)
    slot_ids = set_ids * VIEWS + row_ids // HW % VIEWS
    flat_views = view_ids.reshape(-1)
    slot_range = jnp.arange(flat_views.shape[0], dtype=jnp.int32)
    pose_ids = jnp.sum(
        jnp.where(slot_ids[:, None] == slot_range[None, :], flat_views[None, :], 0), axis=1
    )
    set_range = jnp.arange(time_ids.shape[0], dtype=jnp.int32)
    step_ids = jnp.sum(
        jnp.where(set_ids[:, None] == set_range[None, :], time_ids[None, :], 0), axis=1
    )
    pose_range = jnp.arange(camera_table.shape[0], dtype=jnp.int32)
    onehot_pose = (pose_ids[:, None] == pose_range[None, :]).astype(jnp.float32)
    camera = jnp.dot(onehot_pose, camera_table, precision=lax.Precision.HIGHEST)
    return camera + time_code(step_ids, camera_table.shape[1])


CLASSES = (("xyz", 9), ("yxz", 9), ("zxy", 31), ("zyx", 31))


def class_columns(width):
    total = sum(share for _, share in CLASSES)
    lanes = width // 128
    bounds, spent = [0], 0
    for _, share in CLASSES:
        spent += share
        bounds.append(lanes * spent // total * 128)
    return [(bounds[i], bounds[i + 1] - bounds[i]) for i in range(len(CLASSES))]


def routes(lengths):
    found = []
    for kind, (order, _) in enumerate(CLASSES):
        spans = {axis: range(1 - lengths[axis], lengths[axis]) for axis in "yz"}
        spans["x"] = range(0, 2)
        for dx in spans["x"]:
            for dy in spans["y"]:
                for dz in spans["z"]:
                    hops = abs(dx) + abs(dy) + abs(dz)
                    found.append((hops, kind, {"x": dx, "y": dy, "z": dz}))
    found.sort(key=lambda item: item[0])
    return found


def send_plan(lengths):
    plan = []
    for hops, kind, offset in routes(lengths):
        order = CLASSES[kind][0]
        last = max([i for i in range(3) if offset[order[i]] != 0], default=-1)
        targets = []
        if last >= 0 and order[last] != "x":
            targets.append((order[last], 1 if offset[order[last]] < 0 else -1))
        for axis in order[last + 1 :]:
            targets += [("x", 1)] if axis == "x" else [(axis, 1), (axis, -1)]
        targets.append(("core", 1))
        plan.append((hops, kind, offset, targets))
    return plan


def gather_kernel(lengths, layers, packed_ref, *refs):
    full_refs = refs[:layers]
    own_sem, send_sems, recv_sems = refs[layers:]
    tp_count = lengths["z"]
    rep_here = lax.axis_index("rep")
    here = {
        "z": lax.axis_index("tp"),
        "y": rep_here // 4,
        "x": rep_here // 2 % 2,
        "core": rep_here % 2,
    }
    columns = class_columns(packed_ref.shape[2])

    def device(place):
        return (place["y"] * 4 + place["x"] * 2 + place["core"], place["z"])

    def moved(place, axis, step):
        place = dict(place)
        place[axis] = 1 - place[axis] if axis in ("x", "core") else place[axis] + step
        return place

    def exists(axis, step):
        if axis in ("x", "core"):
            return None
        return here[axis] < lengths[axis] - 1 if step > 0 else here[axis] > 0

    def both(first, second):
        if first is None or second is None:
            return second if first is None else first
        return jnp.logical_and(first, second)

    def guarded(condition, action):
        if condition is None:
            action()
        else:
            pl.when(condition)(action)

    barrier = pltpu.get_barrier_semaphore()
    neighbours = [("core", 1), ("x", 1), ("y", 1), ("y", -1), ("z", 1), ("z", -1)]
    for axis, step in neighbours:
        def greet(axis=axis, step=step):
            pl.semaphore_signal(
                barrier, inc=1, device_id=device(moved(here, axis, step)),
                device_id_type=pl.DeviceIdType.MESH,
            )
        guarded(exists(axis, step), greet)
    count = jnp.int32(2)
    for axis in "yz":
        count = count + (here[axis] > 0).astype(jnp.int32)
        count = count + (here[axis] < lengths[axis] - 1).astype(jnp.int32)
    pl.semaphore_wait(barrier, count)

    my_rep, my_tp = device(here)
    own_copies = [
        pltpu.make_async_copy(
            packed_ref.at[layer], full_refs[layer].at[my_rep * tp_count + my_tp], own_sem.at[layer]
        )
        for layer in range(layers)
    ]
    for copy in own_copies:
        copy.start()

    finish = []
    plan = send_plan(lengths)

    def run(layer, item):
        hops, kind, offset, targets = item
        start, size = columns[kind]
        source = dict(here)
        valid = None
        for axis in "yz":
            source[axis] = here[axis] + offset[axis]
            if offset[axis] > 0:
                valid = both(valid, source[axis] < lengths[axis])
            elif offset[axis] < 0:
                valid = both(valid, source[axis] >= 0)
        if offset["x"]:
            source["x"] = 1 - here["x"]
        rep_from, tp_from = device(source)
        block = rep_from * tp_count + tp_from
        span = pl.ds(start, size)
        landed = full_refs[layer].at[block, :, span]
        origin = packed_ref.at[layer, :, span] if hops == 0 else landed
        arrived = recv_sems.at[layer * len(CLASSES) + kind, block]
        sends = []
        for axis, step in targets:
            copy = pltpu.make_async_remote_copy(
                src_ref=origin,
                dst_ref=landed,
                send_sem=send_sems.at[len(finish) + len(sends)],
                recv_sem=arrived,
                device_id=device(moved(here, axis, step)),
                device_id_type=pl.DeviceIdType.MESH,
            )
            sends.append((both(valid, exists(axis, step)), copy, exists(axis, step)))

        def action():
            if hops:
                sends[-1][1].wait_recv()
            for _, copy, there in sends:
                guarded(there, copy.start)

        guarded(valid, action)
        finish.extend((condition, copy.wait_send) for condition, copy, _ in sends)

        def from_sibling():
            other = dict(source)
            other["core"] = 1 - here["core"]
            rep_other, tp_other = device(other)
            block_other = rep_other * tp_count + tp_other
            there = full_refs[layer].at[block_other, :, span]
            pltpu.make_async_remote_copy(
                src_ref=there,
                dst_ref=there,
                send_sem=send_sems.at[0],
                recv_sem=recv_sems.at[layer * len(CLASSES) + kind, block_other],
                device_id=device(moved(here, "core", 1)),
                device_id_type=pl.DeviceIdType.MESH,
            ).wait_recv()

        finish.append((valid, from_sibling))

    own = [item for item in plan if item[0] == 0]
    rest = [item for item in plan if item[0] > 0]
    for item in own:
        run(0, item)
    for layer in range(layers):
        early = len(rest) // 2
        for item in rest[:early]:
            run(layer, item)
        if layer + 1 < layers:
            for item in own:
                run(layer + 1, item)
        for item in rest[early:]:
            run(layer, item)
    for condition, action in finish:
        guarded(condition, action)
    for copy in own_copies:
        copy.wait()


def gather_weights(packed, rep_count, tp_count):
    layers, rows, width = packed.shape
    devices = rep_count * tp_count
    lengths = {"x": 2, "y": rep_count // 4, "z": tp_count}
    slots = layers * sum(len(item[3]) + 1 for item in send_plan(lengths))
    full = pl.pallas_call(
        functools.partial(gather_kernel, lengths, layers),
        out_shape=[jax.ShapeDtypeStruct((devices, rows, width), packed.dtype)] * layers,
        in_specs=[pl.BlockSpec(memory_space=pltpu.VMEM)],
        out_specs=[pl.BlockSpec(memory_space=pl.ANY)] * layers,
        scratch_shapes=[
            pltpu.SemaphoreType.DMA((layers,)),
            pltpu.SemaphoreType.DMA((slots,)),
            pltpu.SemaphoreType.DMA((layers * len(CLASSES), devices)),
        ],
        compiler_params=pltpu.CompilerParams(collective_id=0, has_side_effects=True),
        name="gather_weights",
    )(packed)
    return [one.reshape(devices * rows, width) for one in full]


def attend(packed, head_size):
    total_rows = packed.shape[0]
    width = packed.shape[1] // 3
    set_rows = VIEWS * HW
    query_rows, sources = packed[:, :width], packed[:, width:]
    if total_rows % set_rows != 0:
        first = lax.axis_index("tp") * total_rows // set_rows * set_rows
        sources = lax.all_gather(sources, "tp", axis=0, tiled=True)
        sources = lax.dynamic_slice_in_dim(sources, first, set_rows, 0)
    set_count = sources.shape[0] // set_rows
    query_rows = query_rows.reshape(set_count, -1, width // head_size, head_size)
    key_rows = sources[:, :width].reshape(set_count, set_rows, -1, head_size)
    value_rows = sources[:, width:].reshape(set_count, set_rows, -1, head_size)
    scores = jnp.einsum(
        "bqhd,bkhd->bhqk", query_rows, key_rows, preferred_element_type=jnp.float32
    ) * head_size ** (-0.5)
    peak = jnp.max(scores, axis=-1, keepdims=True)
    expons = jnp.exp(scores - peak)
    attn_probs = (expons / jnp.sum(expons, axis=-1, keepdims=True)).astype(jnp.bfloat16)
    mixed_rows = jnp.einsum(
        "bhqk,bkhd->bqhd", attn_probs, value_rows, preferred_element_type=jnp.float32
    )
    return mixed_rows.astype(jnp.bfloat16).reshape(total_rows, width)


def out_terms(mixed_rows, weight):
    return lax.dot_general(
        mixed_rows, weight, (((1,), (1,)), ((), ())), preferred_element_type=jnp.float32
    )


def body(
    tokens,
    view_ids,
    time_ids,
    camera_table,
    norm_attn,
    norm_ffn,
    w_query,
    w_key,
    w_value,
    w_out,
    w_gate,
    w_up,
    w_down,
):
    tp_count = lax.axis_size("tp")
    rep_count = lax.axis_size("rep")
    width = w_query.shape[2]
    inner = w_gate.shape[2]
    head_size = D // HEADS
    shards = (w_query, w_key, w_value, w_out, w_gate, w_up, w_down)
    one_kernel = rep_count % 4 == 0 and rep_count * tp_count * LAYERS * len(CLASSES) <= 256
    if one_kernel:
        weights = gather_weights(jnp.concatenate(shards, axis=2), rep_count, tp_count)
    share_rows = tokens.shape[0]
    row_ids = lax.axis_index("tp") * share_rows + jnp.arange(share_rows, dtype=jnp.int32)
    stream = tokens.astype(jnp.float32) + conditioning(row_ids, view_ids, time_ids, camera_table)

    def whole_weight(layer_index, first, count, after):
        if one_kernel:
            start = sum(shard.shape[2] for shard in shards[:first])
            size = sum(shard.shape[2] for shard in shards[first : first + count])
            return weights[layer_index][:, start : start + size]
        own = [shard[layer_index] for shard in shards[first : first + count]]
        own, _ = lax.optimization_barrier((own, after))
        return lax.all_gather(jnp.concatenate(own, axis=1), ("rep", "tp"), axis=0, tiled=True)

    for layer_index in range(LAYERS):
        normed = layer_norm(stream, norm_attn[layer_index])
        qkv_w = whole_weight(layer_index, 0, 3, normed)
        packed = jnp.dot(normed, qkv_w, preferred_element_type=jnp.float32).astype(jnp.bfloat16)
        mixed_rows = attend(packed, head_size)
        stream = stream + out_terms(mixed_rows, whole_weight(layer_index, 3, 1, mixed_rows))
        normed = layer_norm(stream, norm_ffn[layer_index])
        gate_w = whole_weight(layer_index, 4, 1, normed)
        gate_part = jnp.dot(normed, gate_w, preferred_element_type=jnp.float32)
        up_w = whole_weight(layer_index, 5, 1, gate_part)
        up_part = jnp.dot(normed, up_w, preferred_element_type=jnp.float32)
        hidden = (jax.nn.gelu(gate_part, approximate=False) * up_part).astype(jnp.bfloat16)
        stream = stream + out_terms(hidden, whole_weight(layer_index, 6, 1, hidden))
    return stream.astype(jnp.bfloat16)


def solution(mesh):
    return jax.shard_map(
        body,
        mesh=mesh,
        in_specs=(
            P(("rep", "tp"), None),
            P("rep", None),
            P("rep"),
            P(),
            P(),
            P(),
            P(None, ("rep", "tp"), None),
            P(None, ("rep", "tp"), None),
            P(None, ("rep", "tp"), None),
            P(None, ("rep", "tp"), None),
            P(None, ("rep", "tp"), None),
            P(None, ("rep", "tp"), None),
            P(None, ("rep", "tp"), None),
        ),
        out_specs=P(("rep", "tp"), None),
        check_vma=False,
    )
```

```python
import functools
import math

import jax
import jax.numpy as jnp
from jax import lax
from jax.experimental import pallas as pl
from jax.experimental.pallas import tpu as pltpu
from jax.sharding import PartitionSpec as P

D = 1280
HEADS = 8
VIEWS = 4
HW = 64
LAYERS = 2


def layer_norm(activations, gain_vector):
    average = jnp.mean(activations, axis=-1, keepdims=True)
    centred = activations - average
    spread = jnp.mean(centred * centred, axis=-1, keepdims=True)
    return (centred * lax.rsqrt(spread + 1e-05) * gain_vector).astype(jnp.bfloat16)


def time_code(step_ids, width):
    half_width = width // 2
    frequency = jnp.exp(-math.log(10000.0) * jnp.arange(half_width, dtype=jnp.float32) / half_width)
    angles = step_ids.astype(jnp.float32)[:, None] * frequency[None, :]
    return jnp.concatenate([jnp.cos(angles), jnp.sin(angles)], axis=1)


def conditioning(row_ids, view_ids, time_ids, camera_table):
    set_ids = row_ids // (VIEWS * HW)
    slot_ids = set_ids * VIEWS + row_ids // HW % VIEWS
    flat_views = view_ids.reshape(-1)
    slot_range = jnp.arange(flat_views.shape[0], dtype=jnp.int32)
    pose_ids = jnp.sum(
        jnp.where(slot_ids[:, None] == slot_range[None, :], flat_views[None, :], 0), axis=1
    )
    set_range = jnp.arange(time_ids.shape[0], dtype=jnp.int32)
    step_ids = jnp.sum(
        jnp.where(set_ids[:, None] == set_range[None, :], time_ids[None, :], 0), axis=1
    )
    pose_range = jnp.arange(camera_table.shape[0], dtype=jnp.int32)
    onehot_pose = (pose_ids[:, None] == pose_range[None, :]).astype(jnp.float32)
    camera = jnp.dot(onehot_pose, camera_table, precision=lax.Precision.HIGHEST)
    return camera + time_code(step_ids, camera_table.shape[1])


CLASSES = (("xyz", 9), ("yxz", 9), ("zxy", 31), ("zyx", 31))


def class_columns(width):
    total = sum(share for _, share in CLASSES)
    lanes = width // 128
    bounds, spent = [0], 0
    for _, share in CLASSES:
        spent += share
        bounds.append(lanes * spent // total * 128)
    return [(bounds[i], bounds[i + 1] - bounds[i]) for i in range(len(CLASSES))]


def routes(lengths):
    found = []
    for kind, (order, _) in enumerate(CLASSES):
        spans = {axis: range(1 - lengths[axis], lengths[axis]) for axis in "yz"}
        spans["x"] = range(0, 2)
        for dx in spans["x"]:
            for dy in spans["y"]:
                for dz in spans["z"]:
                    hops = abs(dx) + abs(dy) + abs(dz)
                    found.append((hops, kind, {"x": dx, "y": dy, "z": dz}))
    found.sort(key=lambda item: item[0])
    return found


def send_plan(lengths):
    plan = []
    for hops, kind, offset in routes(lengths):
        order = CLASSES[kind][0]
        last = max([i for i in range(3) if offset[order[i]] != 0], default=-1)
        targets = []
        if last >= 0 and order[last] != "x":
            targets.append((order[last], 1 if offset[order[last]] < 0 else -1))
        for axis in order[last + 1 :]:
            targets += [("x", 1)] if axis == "x" else [(axis, 1), (axis, -1)]
        targets.append(("core", 1))
        plan.append((hops, kind, offset, targets))
    return plan


def gather_kernel(lengths, layers, shard_count, *refs):
    shard_refs, full_refs = refs[:shard_count], refs[shard_count : shard_count + layers]
    packed_ref, pack_sem, own_sem, send_sems, recv_sems = refs[shard_count + layers :]
    packing, column = [], 0
    for index, shard_ref in enumerate(shard_refs):
        size = shard_ref.shape[2]
        packing.append(
            pltpu.make_async_copy(
                shard_ref, packed_ref.at[:, :, pl.ds(column, size)], pack_sem.at[index]
            )
        )
        packing[-1].start()
        column += size
    tp_count = lengths["z"]
    rep_here = lax.axis_index("rep")
    here = {
        "z": lax.axis_index("tp"),
        "y": rep_here // 4,
        "x": rep_here // 2 % 2,
        "core": rep_here % 2,
    }
    columns = class_columns(packed_ref.shape[2])

    def device(place):
        return (place["y"] * 4 + place["x"] * 2 + place["core"], place["z"])

    def moved(place, axis, step):
        place = dict(place)
        place[axis] = 1 - place[axis] if axis in ("x", "core") else place[axis] + step
        return place

    def exists(axis, step):
        if axis in ("x", "core"):
            return None
        return here[axis] < lengths[axis] - 1 if step > 0 else here[axis] > 0

    def both(first, second):
        if first is None or second is None:
            return second if first is None else first
        return jnp.logical_and(first, second)

    def guarded(condition, action):
        if condition is None:
            action()
        else:
            pl.when(condition)(action)

    barrier = pltpu.get_barrier_semaphore()
    neighbours = [("core", 1), ("x", 1), ("y", 1), ("y", -1), ("z", 1), ("z", -1)]
    for axis, step in neighbours:
        def greet(axis=axis, step=step):
            pl.semaphore_signal(
                barrier, inc=1, device_id=device(moved(here, axis, step)),
                device_id_type=pl.DeviceIdType.MESH,
            )
        guarded(exists(axis, step), greet)
    count = jnp.int32(2)
    for axis in "yz":
        count = count + (here[axis] > 0).astype(jnp.int32)
        count = count + (here[axis] < lengths[axis] - 1).astype(jnp.int32)
    pl.semaphore_wait(barrier, count)

    for copy in packing:
        copy.wait()
    my_rep, my_tp = device(here)
    own_copies = [
        pltpu.make_async_copy(
            packed_ref.at[layer], full_refs[layer].at[my_rep * tp_count + my_tp], own_sem.at[layer]
        )
        for layer in range(layers)
    ]
    for copy in own_copies:
        copy.start()

    finish = []
    plan = send_plan(lengths)

    def run(layer, item):
        hops, kind, offset, targets = item
        start, size = columns[kind]
        source = dict(here)
        valid = None
        for axis in "yz":
            source[axis] = here[axis] + offset[axis]
            if offset[axis] > 0:
                valid = both(valid, source[axis] < lengths[axis])
            elif offset[axis] < 0:
                valid = both(valid, source[axis] >= 0)
        if offset["x"]:
            source["x"] = 1 - here["x"]
        rep_from, tp_from = device(source)
        block = rep_from * tp_count + tp_from
        span = pl.ds(start, size)
        landed = full_refs[layer].at[block, :, span]
        origin = packed_ref.at[layer, :, span] if hops == 0 else landed
        arrived = recv_sems.at[layer * len(CLASSES) + kind, block]
        sends = []
        for axis, step in targets:
            copy = pltpu.make_async_remote_copy(
                src_ref=origin,
                dst_ref=landed,
                send_sem=send_sems.at[len(finish) + len(sends)],
                recv_sem=arrived,
                device_id=device(moved(here, axis, step)),
                device_id_type=pl.DeviceIdType.MESH,
            )
            sends.append((both(valid, exists(axis, step)), copy, exists(axis, step)))

        def action():
            if hops:
                sends[-1][1].wait_recv()
            for _, copy, there in sends:
                guarded(there, copy.start)

        guarded(valid, action)
        finish.extend((condition, copy.wait_send) for condition, copy, _ in sends)

        def from_sibling():
            other = dict(source)
            other["core"] = 1 - here["core"]
            rep_other, tp_other = device(other)
            block_other = rep_other * tp_count + tp_other
            there = full_refs[layer].at[block_other, :, span]
            pltpu.make_async_remote_copy(
                src_ref=there,
                dst_ref=there,
                send_sem=send_sems.at[0],
                recv_sem=recv_sems.at[layer * len(CLASSES) + kind, block_other],
                device_id=device(moved(here, "core", 1)),
                device_id_type=pl.DeviceIdType.MESH,
            ).wait_recv()

        finish.append((valid, from_sibling))

    own = [item for item in plan if item[0] == 0]
    rest = [item for item in plan if item[0] > 0]
    for item in own:
        run(0, item)
    for layer in range(layers):
        early = len(rest) // 5
        for item in rest[:early]:
            run(layer, item)
        if layer + 1 < layers:
            for item in own:
                run(layer + 1, item)
        for item in rest[early:]:
            run(layer, item)
    for condition, action in finish:
        guarded(condition, action)
    for copy in own_copies:
        copy.wait()


def gather_weights(shards, rep_count, tp_count):
    layers, rows, _ = shards[0].shape
    width = sum(shard.shape[2] for shard in shards)
    kind = shards[0].dtype
    devices = rep_count * tp_count
    lengths = {"x": 2, "y": rep_count // 4, "z": tp_count}
    slots = layers * sum(len(item[3]) + 1 for item in send_plan(lengths))
    full = pl.pallas_call(
        functools.partial(gather_kernel, lengths, layers, len(shards)),
        out_shape=[jax.ShapeDtypeStruct((devices, rows, width), kind)] * layers,
        in_specs=[pl.BlockSpec(memory_space=pl.ANY)] * len(shards),
        out_specs=[pl.BlockSpec(memory_space=pl.ANY)] * layers,
        scratch_shapes=[
            pltpu.VMEM((layers, rows, width), kind),
            pltpu.SemaphoreType.DMA((len(shards),)),
            pltpu.SemaphoreType.DMA((layers,)),
            pltpu.SemaphoreType.DMA((slots,)),
            pltpu.SemaphoreType.DMA((layers * len(CLASSES), devices)),
        ],
        compiler_params=pltpu.CompilerParams(collective_id=0, has_side_effects=True),
        name="gather_weights",
    )(*shards)
    return [one.reshape(devices * rows, width) for one in full]


def attend(packed, head_size):
    total_rows = packed.shape[0]
    width = packed.shape[1] // 3
    set_rows = VIEWS * HW
    query_rows, sources = packed[:, :width], packed[:, width:]
    if total_rows % set_rows != 0:
        first = lax.axis_index("tp") * total_rows // set_rows * set_rows
        sources = lax.all_gather(sources, "tp", axis=0, tiled=True)
        sources = lax.dynamic_slice_in_dim(sources, first, set_rows, 0)
    set_count = sources.shape[0] // set_rows
    query_rows = query_rows.reshape(set_count, -1, width // head_size, head_size)
    key_rows = sources[:, :width].reshape(set_count, set_rows, -1, head_size)
    value_rows = sources[:, width:].reshape(set_count, set_rows, -1, head_size)
    scores = jnp.einsum(
        "bqhd,bkhd->bhqk", query_rows, key_rows, preferred_element_type=jnp.float32
    ) * head_size ** (-0.5)
    peak = jnp.max(scores, axis=-1, keepdims=True)
    expons = jnp.exp(scores - peak)
    attn_probs = (expons / jnp.sum(expons, axis=-1, keepdims=True)).astype(jnp.bfloat16)
    mixed_rows = jnp.einsum(
        "bhqk,bkhd->bqhd", attn_probs, value_rows, preferred_element_type=jnp.float32
    )
    return mixed_rows.astype(jnp.bfloat16).reshape(total_rows, width)


def out_terms(mixed_rows, weight):
    return lax.dot_general(
        mixed_rows, weight, (((1,), (1,)), ((), ())), preferred_element_type=jnp.float32
    )


def ffn_kernel(steps, stream_ref, gain_ref, gate_ref, up_ref, down_ref, out_ref, normed, total):
    step = pl.program_id(0)

    @pl.when(step == 0)
    def _():
        normed[...] = layer_norm(stream_ref[...], gain_ref[...])
        total[...] = stream_ref[...]

    gate_part = jnp.dot(normed[...], gate_ref[...], preferred_element_type=jnp.float32)
    up_part = jnp.dot(normed[...], up_ref[...], preferred_element_type=jnp.float32)
    gate_part = 0.5 * gate_part * (1.0 + lax.erf(gate_part * math.sqrt(0.5)))
    hidden = (gate_part * up_part).astype(jnp.bfloat16)
    total[...] += out_terms(hidden, down_ref[...])

    @pl.when(step == steps - 1)
    def _():
        out_ref[...] = total[...].astype(out_ref.dtype)


def feed_forward(stream, gain_vector, weights, first, inner, out_dtype):
    rows, width = stream.shape
    tile = 512 if inner % 512 == 0 and first % 512 == 0 else 128
    steps = inner // tile
    depth = weights.shape[0]

    def columns(which):
        base = (first + which * inner) // tile
        return pl.BlockSpec((depth, tile), lambda step: (0, base + step))

    return pl.pallas_call(
        functools.partial(ffn_kernel, steps),
        grid=(steps,),
        out_shape=jax.ShapeDtypeStruct((rows, width), out_dtype),
        in_specs=[
            pl.BlockSpec((rows, width), lambda step: (0, 0)),
            pl.BlockSpec((1, width), lambda step: (0, 0)),
            columns(0),
            columns(1),
            columns(2),
        ],
        out_specs=pl.BlockSpec((rows, width), lambda step: (0, 0)),
        scratch_shapes=[
            pltpu.VMEM((rows, width), jnp.bfloat16),
            pltpu.VMEM((rows, width), jnp.float32),
        ],
        compiler_params=pltpu.CompilerParams(dimension_semantics=("arbitrary",)),
        cost_estimate=pl.CostEstimate(
            flops=6 * rows * width * inner,
            bytes_accessed=6 * depth * inner,
            transcendentals=rows * inner,
        ),
        name="feed_forward",
    )(stream, gain_vector[None], weights, weights, weights)


def body(
    tokens,
    view_ids,
    time_ids,
    camera_table,
    norm_attn,
    norm_ffn,
    w_query,
    w_key,
    w_value,
    w_out,
    w_gate,
    w_up,
    w_down,
):
    tp_count = lax.axis_size("tp")
    rep_count = lax.axis_size("rep")
    width = w_query.shape[2]
    inner = w_gate.shape[2]
    head_size = D // HEADS
    shards = (w_query, w_key, w_value, w_out, w_gate, w_up, w_down)
    one_kernel = rep_count % 4 == 0 and rep_count * tp_count * LAYERS * len(CLASSES) <= 256
    if one_kernel:
        weights = gather_weights(shards, rep_count, tp_count)
    share_rows = tokens.shape[0]
    row_ids = lax.axis_index("tp") * share_rows + jnp.arange(share_rows, dtype=jnp.int32)
    stream = tokens.astype(jnp.float32) + conditioning(row_ids, view_ids, time_ids, camera_table)

    def whole_weight(layer_index, first, count, after):
        if one_kernel:
            start = sum(shard.shape[2] for shard in shards[:first])
            size = sum(shard.shape[2] for shard in shards[first : first + count])
            return weights[layer_index][:, start : start + size]
        own = [shard[layer_index] for shard in shards[first : first + count]]
        own, _ = lax.optimization_barrier((own, after))
        return lax.all_gather(jnp.concatenate(own, axis=1), ("rep", "tp"), axis=0, tiled=True)

    for layer_index in range(LAYERS):
        normed = layer_norm(stream, norm_attn[layer_index])
        qkv_w = whole_weight(layer_index, 0, 3, normed)
        packed = jnp.dot(normed, qkv_w, preferred_element_type=jnp.float32).astype(jnp.bfloat16)
        mixed_rows = attend(packed, head_size)
        stream = stream + out_terms(mixed_rows, whole_weight(layer_index, 3, 1, mixed_rows))
        if one_kernel:
            stream = feed_forward(
                stream,
                norm_ffn[layer_index],
                weights[layer_index],
                4 * width,
                inner,
                jnp.bfloat16 if layer_index == LAYERS - 1 else jnp.float32,
            )
            continue
        normed = layer_norm(stream, norm_ffn[layer_index])
        gate_w = whole_weight(layer_index, 4, 1, normed)
        gate_part = jnp.dot(normed, gate_w, preferred_element_type=jnp.float32)
        up_w = whole_weight(layer_index, 5, 1, gate_part)
        up_part = jnp.dot(normed, up_w, preferred_element_type=jnp.float32)
        hidden = (jax.nn.gelu(gate_part, approximate=False) * up_part).astype(jnp.bfloat16)
        stream = stream + out_terms(hidden, whole_weight(layer_index, 6, 1, hidden))
    return stream.astype(jnp.bfloat16)


def solution(mesh):
    return jax.shard_map(
        body,
        mesh=mesh,
        in_specs=(
            P(("rep", "tp"), None),
            P("rep", None),
            P("rep"),
            P(),
            P(),
            P(),
            P(None, ("rep", "tp"), None),
            P(None, ("rep", "tp"), None),
            P(None, ("rep", "tp"), None),
            P(None, ("rep", "tp"), None),
            P(None, ("rep", "tp"), None),
            P(None, ("rep", "tp"), None),
            P(None, ("rep", "tp"), None),
        ),
        out_specs=P(("rep", "tp"), None),
        check_vma=False,
    )
```
